32 devices in a mesh: dp: 4 (over y, core), seq: 8 (over z, x).
Axes of the slice: x: 2, y: 2, z: 4, core: 2. Of those that a mesh axis runs over, the one named last changes fastest.
Arguments:
- queries: bfloat16 [4, 4096, 1024], P('dp', 'seq'), may hold values from -6 to 6
- key_vectors: bfloat16 [4, 4096, 1024], P('dp', 'seq'), may hold values from -6 to 6
- value_vectors: bfloat16 [4, 4096, 2048], P('dp', 'seq'), may hold values from -6 to 6
- grad_output: bfloat16 [4, 4096, 2048], P('dp', 'seq'), may hold values from -0.375 to 0.375
- log_gate: float32 [4, 4096, 1024], P('dp', 'seq'), may hold values from -1 to 0, as said below
- layer_input: bfloat16 [4, 4096, 2048], P('dp', 'seq'), may hold values from -0.0625 to 0.0625
Outputs:
- grad_queries: bfloat16 [4, 4096, 1024], P('dp', 'seq')
- grad_keys: bfloat16 [4, 4096, 1024], P('dp', 'seq')
- grad_values: bfloat16 [4, 4096, 2048], P('dp', 'seq')
- grad_log_gate: float32 [4, 4096, 1024], P('dp', 'seq')
- grad_key_weight: float32 [2048, 1024], P(('dp', 'seq'))
The draws below stay inside these ranges and needn't reach their ends.
Inputs may be any that keep to these rules, and one draw needn't show every extreme that they name: `log_gate`: every entry is negative.
All inputs are finite; a program needn't handle non-finite values.
Results may differ from the reference program's by a relative error of at most 0.03.
Values sent between devices are 32-bit elements; how exact they have to be, the bound alone decides.
A program may use at most 192 MiB of HBM per device.

```python
import jax
import jax.numpy as jnp
from jax import lax

D = 2048
HEADS = 4
DK = 256
DV = 512
GROUP = 64
TOK_DEV = 512
BATCH_SEQUENCES = 4
SEQUENCE_LENGTH = 4096


def draw_log_gate(key, part):
    width = HEADS * DK
    blocks = SEQUENCE_LENGTH // TOK_DEV
    portion_random_key, gradual_random_key, quick_random_key, device_random_key, coarse_random_key, spike_random_key, objective_random_key, regime_random_key = jax.random.split(key, 8)
    share = 0.5
    rough = jnp.exp(jax.random.uniform(coarse_random_key, (BATCH_SEQUENCES, blocks, TOK_DEV, width), jnp.float32, jnp.log(0.6), jnp.log(1.6)))
    slow_mask = jax.random.bernoulli(portion_random_key, share, (BATCH_SEQUENCES, 1, 1, width))
    fast_here = jax.random.bernoulli(regime_random_key, 0.5, (BATCH_SEQUENCES, blocks, 1, width))
    stays_slow = jnp.logical_or(slow_mask, jnp.logical_not(fast_here))
    slow_rate = jnp.exp(jax.random.uniform(gradual_random_key, (BATCH_SEQUENCES, 1, 1, width), jnp.float32, jnp.log(0.02), jnp.log(0.2))) * jnp.log(10.0) / SEQUENCE_LENGTH
    fast_rate = jnp.exp(jax.random.uniform(quick_random_key, (BATCH_SEQUENCES, 1, 1, width), jnp.float32, jnp.log(1.0 / 50.0), jnp.log(1.0 / 30.0)))
    base_rate = jnp.where(stays_slow, slow_rate, fast_rate)
    device_factor = jnp.exp(jax.random.uniform(device_random_key, (BATCH_SEQUENCES, blocks, 1, width), jnp.float32, jnp.log(0.7), jnp.log(1.4)))
    rate_full = (base_rate * device_factor * rough).reshape(BATCH_SEQUENCES, SEQUENCE_LENGTH, width)
    spike_position = jax.random.randint(spike_random_key, (BATCH_SEQUENCES, 3), 0, SEQUENCE_LENGTH)
    position_index = lax.broadcasted_iota(jnp.int32, (BATCH_SEQUENCES, SEQUENCE_LENGTH), 1)
    affected_rows = jnp.any(position_index[:, :, None] == spike_position[:, None, :], axis=2)
    losses = jax.random.uniform(objective_random_key, (BATCH_SEQUENCES, SEQUENCE_LENGTH, width), jnp.float32, jnp.log(0.4), jnp.log(0.8))
    return (jnp.where(affected_rows[:, :, None], losses, 0.0) - rate_full).astype(jnp.float32)


def spiked(values, key, source, target, blocks, factor):
    def block_of(dim):
        return (jnp.arange(values.shape[dim]) // (values.shape[dim] // blocks)).reshape((-1,) + (1,) * (values.ndim - 1 - dim))

    first = jax.random.permutation(key, blocks)[block_of(target)]
    second = (block_of(target) + blocks // 2) % blocks
    return jnp.where((block_of(source) == first) | (block_of(source) == second), factor * values, values)


def shard_levels(rng, dims, cuts, least, largest):
    factor_of, own = 1.0, jax.random.fold_in(rng, 6)
    for position, blocks in cuts:
        steps = jnp.exp(jax.random.uniform(jax.random.fold_in(own, position), (blocks,), jnp.float32, least / len(cuts), largest / len(cuts)))
        factor_of = factor_of * jnp.repeat(steps, dims[position] // blocks).reshape([-1 if axis == position else 1 for axis in range(len(dims))])
    return factor_of


def bell_draw(stream_key, dims, spread, most, cuts=(), held_as=jnp.bfloat16):
    values = jax.random.normal(stream_key, dims, jnp.float32) * spread
    if len(cuts) > 0:
        values = shard_levels(stream_key, dims, cuts, -0.22, 0.18) * values
    return jnp.clip(values, min=-most, max=most).astype(held_as)


def heavy_noise(own_key, extent, spread, limit, pieces, heavy, held_as=jnp.bfloat16):
    drawn = spread * jax.random.normal(own_key, extent, jnp.float32)
    if pieces:
        drawn = drawn * shard_levels(own_key, extent, pieces, -0.22, 0.18)
    return jnp.clip(spiked(drawn, jax.random.fold_in(own_key, 3), *heavy), -limit, limit).astype(held_as)


def setup_inputs(seed: int = 0) -> dict:
    arg_keys = jax.random.split(jax.random.key(seed), 7)
    queries = bell_draw(arg_keys[0], (BATCH_SEQUENCES, SEQUENCE_LENGTH, HEADS * DK), 1.0, 6.0, ((0, 4), (1, 8)))
    key_vectors = bell_draw(arg_keys[1], (BATCH_SEQUENCES, SEQUENCE_LENGTH, HEADS * DK), 1.0, 6.0, ((0, 4), (1, 8)))
    value_vectors = bell_draw(arg_keys[2], (BATCH_SEQUENCES, SEQUENCE_LENGTH, HEADS * DV), 1.0, 6.0, ((0, 4), (1, 8)))
    grad_output = bell_draw(arg_keys[3], (BATCH_SEQUENCES, SEQUENCE_LENGTH, HEADS * DV), (SEQUENCE_LENGTH // 16) ** -0.5, 0.375, ((0, 4), (1, 8)))
    log_gate = draw_log_gate(jax.random.fold_in(arg_keys[6], 71), 0)
    layer_input = heavy_noise(arg_keys[5], (BATCH_SEQUENCES, SEQUENCE_LENGTH, D), (BATCH_SEQUENCES * SEQUENCE_LENGTH) ** -0.5, 0.0625, ((0, 4), (1, 8)), (1, 2, 8, 2.0))
    return {"queries": queries, "key_vectors": key_vectors, "value_vectors": value_vectors, "grad_output": grad_output, "log_gate": log_gate, "layer_input": layer_input}


def widened(first_op, second_op):
    low_pair = lax.optimization_barrier((first_op.astype(jnp.bfloat16), second_op.astype(jnp.bfloat16)))
    return low_pair[0].astype(jnp.float32), low_pair[1].astype(jnp.float32)


def product(pattern, first_op, second_op):
    first_wide, second_wide = widened(first_op, second_op)
    return jnp.einsum(pattern, first_wide, second_wide, precision=lax.Precision.HIGHEST)


def reference(queries, key_vectors, value_vectors, grad_output, log_gate, layer_input):
    blocks = SEQUENCE_LENGTH // GROUP
    key_scale = DK ** -0.5

    def as_blocks(array, width):
        shaped = array.astype(jnp.float32).reshape(BATCH_SEQUENCES, blocks, GROUP, HEADS, width)
        return jnp.transpose(shaped, (1, 0, 2, 3, 4))

    def as_rows(array, width):
        return jnp.transpose(array, (1, 0, 2, 3, 4)).reshape(BATCH_SEQUENCES, SEQUENCE_LENGTH, HEADS * width)

    query_rows = as_blocks(queries, DK)
    key_rows = as_blocks(key_vectors, DK)
    value_rows = as_blocks(value_vectors, DV)
    cotan_rows = as_blocks(grad_output, DV)
    block_cums = jnp.cumsum(as_blocks(log_gate, DK), axis=2)
    lower_mask = (lax.broadcasted_iota(jnp.int32, (GROUP, GROUP), 0) >= lax.broadcasted_iota(jnp.int32, (GROUP, GROUP), 1)).astype(jnp.float32)

    def forward_block(carry_state, block):
        key_part, value_part, cotan_part, cum_part = block
        cum_end = cum_part[:, -1]
        pair_dot = product("bthj,bshj->bhts", cotan_part, value_part) * lower_mask
        grad_q = key_scale * jnp.exp(cum_part) * (product("bthj,bhij->bthi", cotan_part, carry_state) + product("bhts,bshi->bthi", pair_dot, key_part * jnp.exp(-cum_part)))
        carry_state = carry_state * jnp.exp(cum_end)[..., None] + product("bshi,bshj->bhij", key_part * jnp.exp(cum_end[:, None] - cum_part), value_part)
        return carry_state, grad_q

    def backward_block(back_state, block):
        query_part, key_part, value_part, cotan_part, cum_part = block
        cum_end = cum_part[:, -1]
        query_up = query_part * jnp.exp(cum_part)
        key_down = key_part * jnp.exp(-cum_part)
        key_end = key_part * jnp.exp(cum_end[:, None] - cum_part)
        scores = key_scale * product("bthi,bshi->bhts", query_up, key_down) * lower_mask
        pair_dot = product("bthj,bshj->bhts", cotan_part, value_part) * lower_mask
        grad_k = key_scale * jnp.exp(-cum_part) * product("bhts,bthi->bshi", pair_dot, query_up) + jnp.exp(cum_end[:, None] - cum_part) * product("bshj,bhij->bshi", value_part, back_state)
        grad_v = product("bhts,bthj->bshj", scores, cotan_part) + product("bshi,bhij->bshj", key_end, back_state)
        back_state = back_state * jnp.exp(cum_end)[..., None] + key_scale * product("bthi,bthj->bhij", query_up, cotan_part)
        return back_state, (grad_k, grad_v)

    zero_state = jnp.zeros((BATCH_SEQUENCES, HEADS, DK, DV), jnp.float32)
    grad_q = lax.scan(forward_block, zero_state, (key_rows, value_rows, cotan_rows, block_cums))[1]
    grad_k, grad_v = lax.scan(backward_block, zero_state, (query_rows, key_rows, value_rows, cotan_rows, block_cums), reverse=True)[1]
    log_drift = query_rows * grad_q - key_rows * grad_k
    grad_log_gate = lax.cumsum(as_rows(log_drift, DK), axis=1, reverse=True)
    grad_keys = as_rows(grad_k, DK).astype(jnp.bfloat16)
    input_wide = layer_input.reshape(BATCH_SEQUENCES * SEQUENCE_LENGTH, D).astype(jnp.float32)
    keys_wide = grad_keys.reshape(BATCH_SEQUENCES * SEQUENCE_LENGTH, HEADS * DK).astype(jnp.float32)
    grad_key_weight = jnp.dot(jnp.transpose(input_wide), keys_wide, precision=lax.Precision.HIGHEST)
    return (as_rows(grad_q, DK).astype(jnp.bfloat16), grad_keys, as_rows(grad_v, DV).astype(jnp.bfloat16), grad_log_gate, grad_key_weight)
```

```python
import functools

import jax
import jax.numpy as jnp
from jax import lax
from jax.experimental import pallas as pl
from jax.experimental.pallas import tpu as pltpu
from jax.sharding import PartitionSpec as P

HEADS = 4
DK = 256
DV = 512
ROWS = 64
SKEW = 3
AHEAD = 10
LATE = 5
AFTER = ((2, 2), (8, 12), (13, 17), (17, 21), (31, 33))
LANES = 128
NT = (((1,), (1,)), ((), ()))
TN = (((0,), (0,)), ((), ()))
NN = (((1,), (0,)), ((), ()))


def mm(first_op, second_op, dims):
    return lax.dot_general(
        first_op.astype(jnp.bfloat16),
        second_op.astype(jnp.bfloat16),
        dims,
        preferred_element_type=jnp.float32,
    )


def block_of(length):
    return 128 if length % 128 == 0 else 64


def triangle(size, lower):
    row = lax.broadcasted_iota(jnp.int32, (size, size), 0)
    col = lax.broadcasted_iota(jnp.int32, (size, size), 1)
    return (row >= col) if lower else (row <= col)


def exact_sum(ones, values):
    high = values.astype(jnp.bfloat16)
    rest = values - high.astype(jnp.float32)
    middle = rest.astype(jnp.bfloat16)
    low = (rest - middle.astype(jnp.float32)).astype(jnp.bfloat16)
    return mm(ones, high, NN) + (mm(ones, middle, NN) + mm(ones, low, NN))


def bits_of(size):
    return max(size - 1, 0).bit_length()


def sum_stages(sizes):
    wide, high, low = sizes
    made = [("core", 0)]
    for axis, size in (("y", wide), ("a", high), ("b", low)):
        made += [(axis, bit) for bit in range(bits_of(size))]
    return made


def cut(h, width):
    if isinstance(h, int):
        return slice(h * width, (h + 1) * width)
    return pl.ds(pl.multiple_of(h * width, width), width)


def flow_kernel(sizes, *refs):
    given, outs, refs = refs[:6], refs[6:11], refs[11:]
    q_ref, k_ref, v_ref, g_ref, lg_ref, x_ref = refs[:6]
    dq_ref, dk_ref, dv_ref, gate_ref, w_out, near_ref, fin, bin_ = refs[6:14]
    d_all, f_all, b_all, f_row, b_row, part, got, back_ref, state_ref = refs[14:23]
    d_send, d_recv, x_send, x_recv, l_send, l_recv, z_send, z_recv, w_send, w_recv = refs[23:33]
    in_sem, out_sem = refs[33:]
    wide, high, low = sizes
    length = q_ref.shape[0]
    size = block_of(length)
    blocks = length // size
    scale = DK**-0.5
    step_rows = ROWS * max(1, low // 2)
    per_head = DV // step_rows
    slots = 2 * HEADS * per_head
    dp, seq = lax.axis_index("dp"), lax.axis_index("seq")
    me = {"y": dp // 2, "core": dp % 2, "a": seq // low, "b": seq % low}
    a, b = me["a"], me["b"]
    stages = sum_stages(sizes)
    rows = w_out.shape[0]

    def device(**changes):
        place = me | changes
        return {"dp": place["y"] * 2 + place["core"], "seq": place["a"] * low + place["b"]}

    def flipped(axis, bit):
        bit_is = (me[axis] // (1 << bit)) % 2
        return me[axis] + (1 << bit) * (1 - 2 * bit_is), bit_is

    def remote(source, into, send, recv, target):
        return pltpu.make_async_remote_copy(
            src_ref=source,
            dst_ref=into,
            send_sem=send,
            recv_sem=recv,
            device_id=target,
            device_id_type=pl.DeviceIdType.MESH,
        )

    row_peers = [lax.rem(b + k, low) for k in range(1, low)]
    row_from = [lax.rem(b + low - k, low) for k in range(1, low)]

    barrier = pltpu.get_barrier_semaphore()

    def greet(target):
        pl.semaphore_signal(
            barrier, inc=1, device_id=target, device_id_type=pl.DeviceIdType.MESH
        )

    greeted = [device(b=p) for p in row_peers]
    for axis, bit in stages:
        if axis != "b":
            greeted.append(device(**{axis: flipped(axis, bit)[0]}))
    for target in greeted:
        greet(target)
    for ahead in (1, -1):
        near = a + ahead

        @pl.when((near >= 0) & (near < high))
        def _():
            greet(device(a=near))

    def greeting_done():
        near = jnp.where(a > 0, 1, 0) + jnp.where(a < high - 1, 1, 0)
        pl.semaphore_wait(barrier, len(greeted) + near)

    def d_copies():
        return [
            remote(d_all.at[b], d_all.at[b], d_send.at[k], d_recv.at[k], device(b=p))
            for k, p in enumerate(row_peers)
        ]

    def at_chunk(c):
        return pl.ds(pl.multiple_of(c * step_rows, step_rows), step_rows)

    sides = {"F": (0, f_all, f_row, fin), "B": (1, b_all, b_row, bin_)}

    def order_of(kind):
        return list(range(low)) if kind == "F" else list(reversed(range(low)))

    def early(kind, c, owner):
        n, states, _, _ = sides[kind]
        place = states.at[b, at_chunk(c)]
        k = lax.rem(owner + low - b, low) - 1
        return remote(place, place, x_send.at[n, c], x_recv.at[n, k, c], device(b=owner))

    def early_arrival(kind, c, i):
        n, states, _, _ = sides[kind]
        place = states.at[i, at_chunk(c)]
        k = lax.rem(b + low - i, low) - 1
        return remote(place, place, x_send.at[n, c], x_recv.at[n, k, c], device(b=i))

    def late(kind, c, i):
        n, states, _, kept = sides[kind]
        return remote(
            states.at[i, at_chunk(c)],
            kept.at[at_chunk(c)],
            l_send.at[n, lax.rem(i + low - b, low) - 1, c],
            l_recv.at[n, c],
            device(b=i),
        )

    def late_arrival(kind, c):
        n, _, _, kept = sides[kind]
        place = kept.at[at_chunk(c)]
        return remote(place, place, l_send.at[n, 0, c], l_recv.at[n, c], device())

    def needs_early(kind, i, owner):
        last = high - 1 if kind == "F" else 0
        return (i != owner) & ((a != last) | (i != order_of(kind)[-1]))

    def needs_late(kind, i, owner):
        first = 0 if kind == "F" else high - 1
        return (i != owner) & ((a != first) | (i != order_of(kind)[0]))

    def z_copy(kind, c, toward):
        n, _, carried, _ = sides[kind]
        return remote(
            carried.at[at_chunk(c)],
            carried.at[at_chunk(c)],
            z_send.at[n, c],
            z_recv.at[n, c],
            device(a=toward),
        )

    half = HEADS * per_head

    def chunk_of(kind, slot):
        c = slot if kind == "B" else slot - half
        return c, (c >= 0) & (c < half)

    def issue(slot):
        for kind in ("B", "F"):
            c, asked = chunk_of(kind, slot)
            owner = lax.rem((c + 2 * slots) // per_head, low)

            @pl.when(asked & needs_early(kind, b, owner))
            def _():
                early(kind, c, owner).start()

    def serve(kind, slot):
        _, states, carried, kept = sides[kind]
        c, asked = chunk_of(kind, slot)
        head = (c + 2 * slots) // per_head - 2 * slots // per_head
        first, last, ahead = (0, high - 1, 1) if kind == "F" else (high - 1, 0, -1)


        @pl.when(asked & (lax.rem((c + 2 * slots) // per_head, low) == b))
        def _():
            here = at_chunk(c)
            for i in range(low):

                @pl.when(needs_early(kind, i, b))
                def _():
                    early_arrival(kind, c, i).wait_recv()

            @pl.when(a == first)
            def _():
                carried[here, :] = jnp.zeros((step_rows, DK), jnp.float32)

            @pl.when(a != first)
            def _():
                z_copy(kind, c, a).wait_recv()

            current = carried[here, :]
            for i in order_of(kind):
                own = states[i, here, :]
                decay = d_all[i, pl.ds(pl.multiple_of(head * 8, 8), 8), :][0:1, :]

                @pl.when(b == i)
                def _():
                    kept[here, :] = current

                @pl.when(needs_late(kind, i, b))
                def _():
                    states[i, here, :] = current
                    late(kind, c, i).start()

                current = decay * current + own

            @pl.when(a != last)
            def _():
                carried[here, :] = current
                z_copy(kind, c, a + ahead).start()

    def arrived(kind, h):
        owner = lax.rem(h, low)
        _, _, _, kept = sides[kind]

        @pl.when(needs_late(kind, b, owner))
        def _():
            def one(c, _):
                late_arrival(kind, c).wait_recv()
                return 0

            lax.fori_loop(h * per_head, (h + 1) * per_head, one, 0)

        @pl.when((b != owner) & jnp.logical_not(needs_late(kind, b, owner)))
        def _():
            kept[cut(h, DV), :] = jnp.zeros((DV, DK), jnp.float32)

    def tick(t):
        issue(t + AHEAD)
        serve("B", t - SKEW * (high - 1 - a))
        serve("F", t - SKEW * a)

    def states_of(h):
        cols, wide_cols = cut(h, DK), cut(h, DV)
        for one in inputs(h):
            one.wait()
        ones = triangle(size, True).astype(jnp.bfloat16)
        base = jnp.zeros((1, DK), jnp.float32)
        cums = []
        for n in range(blocks):
            made = exact_sum(ones, lg_ref[n * size : (n + 1) * size, cols]) + base
            base = made[size - 1 :, :]
            cums.append(made)
        cum = jnp.concatenate(cums, axis=0)
        query_up = q_ref[:, cols].astype(jnp.float32) * jnp.exp(cum)
        key_end = k_ref[:, cols].astype(jnp.float32) * jnp.exp(base - cum)
        b_all[b, wide_cols, :] = scale * mm(g_ref[:, wide_cols], query_up, TN)
        f_all[b, wide_cols, :] = mm(v_ref[:, wide_cols], key_end, TN)

    def query_block(n, h):
        cols, wide_cols = cut(h, DK), cut(h, DV)
        at = slice(n * size, (n + 1) * size)
        lower = triangle(size, True)
        cum = exact_sum(lower.astype(jnp.bfloat16), lg_ref[at, cols])
        end = cum[size - 1 :, :]
        middle = cum[size // 2 - 1 : size // 2, :]
        key = k_ref[at, cols].astype(jnp.float32)
        pair = jnp.where(lower, mm(g_ref[at, wide_cols], v_ref[at, wide_cols], NT), 0.0)
        near = jnp.exp(cum - middle) * mm(pair, key * jnp.exp(middle - cum), NN)
        if n > 0:
            near += jnp.exp(cum) * mm(g_ref[at, wide_cols], state_ref[...], NN)
        near_ref[at, cols] = scale * near
        if n < blocks - 1:
            added = mm(v_ref[at, wide_cols], key * jnp.exp(end - cum), TN)
            state_ref[...] = state_ref[...] * jnp.exp(end) + added if n > 0 else added

    def key_block(n, h):
        cols, wide_cols = cut(h, DK), cut(h, DV)
        at = slice(n * size, (n + 1) * size)
        lower = triangle(size, True)
        back = bin_[wide_cols, :] if n == blocks - 1 else back_ref[...]
        cum = exact_sum(lower.astype(jnp.bfloat16), lg_ref[at, cols])
        end = cum[size - 1 :, :]
        middle = cum[size // 2 - 1 : size // 2, :]
        fall = jnp.exp(middle - cum)
        to_end = jnp.exp(end - cum)
        query = q_ref[at, cols].astype(jnp.float32)
        key = k_ref[at, cols].astype(jnp.float32)
        query_rise = (query * jnp.exp(cum - middle)).astype(jnp.bfloat16)
        pair = jnp.where(lower, mm(g_ref[at, wide_cols], v_ref[at, wide_cols], NT), 0.0)
        scores = jnp.where(lower, scale * mm(query_rise, key * fall, NT), 0.0)
        dk = scale * fall * mm(pair, query_rise, TN) + to_end * mm(
            v_ref[at, wide_cols], back, NN
        )
        dv = mm(scores, g_ref[at, wide_cols], TN) + mm(key * to_end, back, NT)
        dk_ref[at, cols] = dk.astype(jnp.bfloat16)
        dv_ref[at, wide_cols] = dv.astype(jnp.bfloat16)
        gate_ref[at, cols] = key * dk
        if n > 0:
            back_ref[...] = back * jnp.exp(end) + scale * mm(
                g_ref[at, wide_cols], query * jnp.exp(cum), TN
            )

    def finish(h):
        cols, wide_cols = cut(h, DK), cut(h, DV)
        arrived("F", h)
        sum_down = triangle(size, True).astype(jnp.bfloat16)
        sum_up = triangle(size, False).astype(jnp.bfloat16)
        state = fin[wide_cols, :]
        far = scale * mm(g_ref[:, wide_cols], state, NN)
        base = jnp.zeros((1, DK), jnp.float32)
        kept = []
        for n in range(blocks):
            at = slice(n * size, (n + 1) * size)
            cum = exact_sum(sum_down, lg_ref[at, cols]) + base
            base = cum[size - 1 :, :]
            dq = near_ref[at, cols] + jnp.exp(cum) * far[at, :]
            dq_ref[at, cols] = dq.astype(jnp.bfloat16)
            kept.append(q_ref[at, cols].astype(jnp.float32) * dq - gate_ref[at, cols])
        last = state * jnp.exp(base) + f_all[b, wide_cols, :]
        tail = jnp.sum(last * bin_[wide_cols, :], axis=0, keepdims=True)
        for n in reversed(range(blocks)):
            sums = exact_sum(sum_up, kept[n]) + tail
            gate_ref[n * size : (n + 1) * size, cols] = sums
            tail = sums[0:1, :]
        result(0, h).start()
        result(3, h).start()

    def inputs(h):
        made = []
        for i, width in enumerate((DK, DK, DV, DV)):
            place = (slice(None), cut(h, width))
            made.append(
                pltpu.make_async_copy(
                    given[i].at[place], (q_ref, k_ref, v_ref, g_ref)[i].at[place], in_sem.at[i, h]
                )
            )
        return made

    def result(i, h):
        source = (dq_ref, dk_ref, dv_ref, gate_ref, w_out)[i]
        place = (slice(None), cut(h, DV if i == 2 else DK))
        return pltpu.make_async_copy(source.at[place], outs[i].at[place], out_sem.at[i, h])

    def slot_of(owner):
        place = {
            "b": owner % low,
            "a": owner // low % high,
            "core": owner // (low * high) % 2,
            "y": owner // (low * high * 2),
        }
        slot = 0
        for axis, bit in stages:
            slot = slot * 2 + (place[axis] >> bit) % 2
        return slot

    tall = min(256, x_ref.shape[1])
    tiles = x_ref.shape[1] // tall

    def weight_tile(i, h):
        total = mm(x_ref[:, i * tall : (i + 1) * tall], dk_ref[:, cut(h, DK)], TN)
        for j in range(tall // rows):
            place = slot_of(i * (tall // rows) + j)
            for e in range(2):
                part[h * 2 + e, place] = total[
                    j * rows : (j + 1) * rows, e * LANES : (e + 1) * LANES
                ]

    count = 1 << len(stages)

    def sum_place(s):
        start = 0
        for e, (axis, bit) in enumerate(stages[:s]):
            start = start + flipped(axis, bit)[1] * (count >> (e + 1))
        axis, bit = stages[s]
        peer, mine = flipped(axis, bit)
        n = count >> (s + 1)
        return start + mine * n, start + (1 - mine) * n, n, count - 2 * n, device(**{axis: peer})

    def sum_copy(h, s):
        _, other, n, offset, target = sum_place(s)
        return remote(
            part.at[h, pl.ds(other, n)],
            got.at[h, pl.ds(offset, n)],
            w_send.at[h, s],
            w_recv.at[h, s],
            target,
        )

    def sum_land(e, s, h):
        own, _, n, offset, _ = sum_place(s)
        h = h * 2 + e
        sum_copy(h, s).wait_recv()
        if s == len(stages) - 1:
            w_out[:, cut(h, LANES)] = part[h, own] + got[h, offset]
            return

        def add(j, _):
            part[h, own + j] = part[h, own + j] + got[h, offset + j]
            return 0

        lax.fori_loop(0, n, add, 0)
        sum_copy(h, s + 1).start()

    def key_done(h):
        result(1, h).start()
        result(2, h).start()

    def sum_begin(h):
        for e in range(2):
            sum_copy(h * 2 + e, 0).start()

    def ticks(eighths):
        return eighths * per_head // 8

    events = []
    for n in range(blocks):
        events.append((ticks(8 + 2 * n), functools.partial(query_block, n)))
    key_at = per_head + SKEW * (high - 1) + ticks(LATE)
    todo = [functools.partial(arrived, "B")]
    todo += [functools.partial(key_block, n) for n in reversed(range(blocks))] + [key_done]
    todo += [functools.partial(weight_tile, i) for i in range(tiles)] + [sum_begin]
    for j, one in enumerate(todo):
        events.append((key_at + ticks(j // 3), one))
    sum_at = events[-1][0]
    for s in range(len(stages)):
        for e in range(2):
            spot = AFTER[min(s, len(AFTER) - 2) if s < len(stages) - 1 else -1][e]
            events.append((sum_at + ticks(spot), functools.partial(sum_land, e, s)))
    events.append((half + key_at, finish))
    events.append((events[-2][0] + 1, lambda h: result(4, h).start()))
    events.sort(key=lambda one: (one[0] % per_head, one[0]))
    periods = HEADS + max(one[0] for one in events) // per_head

    def run_ticks(start, stop):
        if isinstance(stop, int) and stop == 1 + start:
            tick(start)
        else:
            lax.fori_loop(start, stop, lambda t, _: (tick(t), 0)[1], 0)

    def period(p, _):
        done = 0
        for offset, act in events:
            upto = offset % per_head
            if upto > done:
                run_ticks(p * per_head + done, p * per_head + upto)
                done = upto
            h = p - offset // per_head

            @pl.when((h >= 0) & (h < HEADS))
            def _():
                act(h)

        run_ticks(p * per_head + done, (p + 1) * per_head)
        return 0

    all_gates = pltpu.make_async_copy(given[4], lg_ref, in_sem.at[4, 0])
    all_rows = pltpu.make_async_copy(given[5], x_ref, in_sem.at[5, 0])
    all_gates.start()
    for h in range(HEADS):
        for one in inputs(h):
            one.start()
    all_rows.start()
    all_gates.wait()
    for h in range(HEADS):
        total = jnp.sum(lg_ref[:, h * DK : (h + 1) * DK], axis=0, keepdims=True)
        d_all[b, h * 8 : (h + 1) * 8, :] = jnp.broadcast_to(jnp.exp(total), (8, DK))
    states_of(0)
    greeting_done()
    for one in d_copies():
        one.start()
    for h in range(HEADS):
        if h > 0:
            states_of(h)
        for slot in range(h * per_head, min(AHEAD, (h + 1) * per_head)):
            issue(slot)
    for k, p in enumerate(row_from):
        remote(d_all.at[p], d_all.at[p], d_send.at[k], d_recv.at[k], device(b=p)).wait_recv()
    all_rows.wait()
    lax.fori_loop(0, periods, period, 0)

    for one in d_copies():
        one.wait_send()

    def drain(c, _):
        owner = lax.rem(c // per_head, low)
        for kind, last, ahead in (("F", high - 1, 1), ("B", 0, -1)):

            @pl.when(needs_early(kind, b, owner))
            def _():
                early(kind, c, owner).wait_send()

            for i in range(low):

                @pl.when((owner == b) & needs_late(kind, i, owner))
                def _():
                    late(kind, c, i).wait_send()

            @pl.when((owner == b) & (a != last))
            def _():
                z_copy(kind, c, a + ahead).wait_send()

        return 0

    lax.fori_loop(0, HEADS * per_head, drain, 0)

    def sent(h, _):
        for s in range(len(stages)):
            for e in range(2):
                sum_copy(h * 2 + e, s).wait_send()
        return 0

    lax.fori_loop(0, HEADS, sent, 0)
    for h in range(HEADS):
        for i in range(5):
            result(i, h).wait()


def shards(counts, queries, key_vectors, value_vectors, grad_output, log_gate, layer_input):
    length = queries.shape[1]
    ranks, count = counts
    f32, bf16 = jnp.float32, jnp.bfloat16
    low = max(d for d in range(1, count + 1) if count % d == 0 and d * d <= count)
    sizes = (ranks // 2, count // low, low)
    model = layer_input.shape[2]
    own_rows = model // (ranks * count)
    chunks = HEADS * DV // (ROWS * max(1, low // 2))
    steps = len(sum_stages(sizes))
    rows = (queries[0], key_vectors[0], value_vectors[0], grad_output[0], log_gate[0])
    outside = pl.BlockSpec(memory_space=pl.ANY)
    state = pltpu.VMEM((HEADS * DV, DK), f32)
    every = pltpu.VMEM((low, HEADS * DV, DK), f32)
    summed = pltpu.VMEM((HEADS * 2, ranks * count, own_rows, LANES), f32)
    dma = pltpu.SemaphoreType.DMA
    peers = max(1, low - 1)
    spread = (length, HEADS * DK)
    values = (length, HEADS * DV)
    shapes = [(spread, bf16), (spread, bf16), (values, bf16), (spread, f32)]
    shapes += [((own_rows, HEADS * DK), f32)]
    grad_q, grad_k, grad_v, grad_gate, grad_key_weight = pl.pallas_call(
        functools.partial(flow_kernel, sizes),
        in_specs=[outside] * 6,
        out_specs=[outside] * 5,
        out_shape=[jax.ShapeDtypeStruct(shape, kind) for shape, kind in shapes],
        scratch_shapes=[pltpu.VMEM(spread, bf16)] * 2
        + [pltpu.VMEM(values, bf16)] * 2
        + [pltpu.VMEM(spread, f32), pltpu.VMEM((length, model), bf16)]
        + [pltpu.VMEM(shape, kind) for shape, kind in shapes]
        + [pltpu.VMEM(spread, f32), state, state]
        + [pltpu.VMEM((low, HEADS * 8, DK), f32), every, every, state, state]
        + [summed, summed, pltpu.VMEM((DV, DK), f32), pltpu.VMEM((DV, DK), f32)]
        + [dma((peers,)), dma((peers,)), dma((2, chunks)), dma((2, peers, chunks))]
        + [dma((2, peers, chunks)), dma((2, chunks)), dma((2, chunks)), dma((2, chunks))]
        + [dma((HEADS * 2, steps)), dma((HEADS * 2, steps)), dma((6, HEADS)), dma((5, HEADS))],
        compiler_params=pltpu.CompilerParams(
            collective_id=0, has_side_effects=True, vmem_limit_bytes=67000000
        ),
        name="flow",
    )(*rows, layer_input[0])
    return (grad_q[None], grad_k[None], grad_v[None], grad_gate[None], grad_key_weight)


def solution(mesh):
    rows = P("dp", "seq", None)
    return jax.shard_map(
        functools.partial(shards, (mesh.shape["dp"], mesh.shape["seq"])),
        mesh=mesh,
        in_specs=(rows,) * 6,
        out_specs=(rows, rows, rows, rows, P(("dp", "seq"), None)),
        check_vma=False,
    )
```

```python
import functools

import jax
import jax.numpy as jnp
from jax import lax
from jax.experimental import pallas as pl
from jax.experimental.pallas import tpu as pltpu
from jax.sharding import PartitionSpec as P

HEADS = 4
DK = 256
DV = 512
ROWS = 64
SKEW = 3
AHEAD = 10
OPENING = 2
FASTER = (1, 1)
LATE = 5
AFTER = ((2, 2), (8, 12), (13, 17), (17, 21), (31, 33))
LANES = 128
NT = (((1,), (1,)), ((), ()))
TN = (((0,), (0,)), ((), ()))
NN = (((1,), (0,)), ((), ()))


def mm(first_op, second_op, dims):
    return lax.dot_general(
        first_op.astype(jnp.bfloat16),
        second_op.astype(jnp.bfloat16),
        dims,
        preferred_element_type=jnp.float32,
    )


def block_of(length):
    return 128 if length % 128 == 0 else 64


def triangle(size, lower):
    row = lax.broadcasted_iota(jnp.int32, (size, size), 0)
    col = lax.broadcasted_iota(jnp.int32, (size, size), 1)
    return (row >= col) if lower else (row <= col)


def exact_sum(ones, values):
    high = values.astype(jnp.bfloat16)
    rest = values - high.astype(jnp.float32)
    middle = rest.astype(jnp.bfloat16)
    low = (rest - middle.astype(jnp.float32)).astype(jnp.bfloat16)
    return mm(ones, high, NN) + (mm(ones, middle, NN) + mm(ones, low, NN))


def bits_of(size):
    return max(size - 1, 0).bit_length()


def sum_stages(sizes):
    wide, high, low = sizes
    made = [("core", 0)]
    for axis, size in (("y", wide), ("a", high), ("b", low)):
        made += [(axis, bit) for bit in range(bits_of(size))]
    return made


def cut(h, width):
    if isinstance(h, int):
        return slice(h * width, (h + 1) * width)
    return pl.ds(pl.multiple_of(h * width, width), width)


def flow_kernel(sizes, *refs):
    given, outs, refs = refs[:6], refs[6:11], refs[11:]
    q_ref, k_ref, v_ref, g_ref, lg_ref, x_ref = refs[:6]
    dq_ref, dk_ref, dv_ref, gate_ref, w_out, near_ref, fin, bin_ = refs[6:14]
    d_all, f_all, b_all, f_row, b_row, part, got, back_ref, state_ref = refs[14:23]
    d_send, d_recv, x_send, x_recv, l_send, l_recv, z_send, z_recv, w_send, w_recv = refs[23:33]
    in_sem, out_sem = refs[33:]
    wide, high, low = sizes
    length = q_ref.shape[0]
    size = block_of(length)
    blocks = length // size
    scale = DK**-0.5
    step_rows = ROWS * max(1, low // 2)
    per_head = DV // step_rows
    slots = 2 * HEADS * per_head
    dp, seq = lax.axis_index("dp"), lax.axis_index("seq")
    me = {"y": dp // 2, "core": dp % 2, "a": seq // low, "b": seq % low}
    a, b = me["a"], me["b"]
    stages = sum_stages(sizes)
    rows = w_out.shape[0]

    def device(**changes):
        place = me | changes
        return {"dp": place["y"] * 2 + place["core"], "seq": place["a"] * low + place["b"]}

    def flipped(axis, bit):
        bit_is = (me[axis] // (1 << bit)) % 2
        return me[axis] + (1 << bit) * (1 - 2 * bit_is), bit_is

    def remote(source, into, send, recv, target):
        return pltpu.make_async_remote_copy(
            src_ref=source,
            dst_ref=into,
            send_sem=send,
            recv_sem=recv,
            device_id=target,
            device_id_type=pl.DeviceIdType.MESH,
        )

    row_peers = [lax.rem(b + k, low) for k in range(1, low)]
    row_from = [lax.rem(b + low - k, low) for k in range(1, low)]

    barrier = pltpu.get_barrier_semaphore()

    def greet(target):
        pl.semaphore_signal(
            barrier, inc=1, device_id=target, device_id_type=pl.DeviceIdType.MESH
        )

    greeted = [device(b=p) for p in row_peers]
    for axis, bit in stages:
        if axis != "b":
            greeted.append(device(**{axis: flipped(axis, bit)[0]}))
    for target in greeted:
        greet(target)
    for ahead in (1, -1):
        near = a + ahead

        @pl.when((near >= 0) & (near < high))
        def _():
            greet(device(a=near))

    def greeting_done():
        near = jnp.where(a > 0, 1, 0) + jnp.where(a < high - 1, 1, 0)
        pl.semaphore_wait(barrier, len(greeted) + near)

    def d_copies():
        return [
            remote(d_all.at[b], d_all.at[b], d_send.at[k], d_recv.at[k], device(b=p))
            for k, p in enumerate(row_peers)
        ]

    def at_chunk(c):
        return pl.ds(pl.multiple_of(c * step_rows, step_rows), step_rows)

    sides = {"F": (0, f_all, f_row, fin), "B": (1, b_all, b_row, bin_)}

    def order_of(kind):
        return list(range(low)) if kind == "F" else list(reversed(range(low)))

    def early(kind, c, owner):
        n, states, _, _ = sides[kind]
        place = states.at[b, at_chunk(c)]
        k = lax.rem(owner + low - b, low) - 1
        return remote(place, place, x_send.at[n, c], x_recv.at[n, k, c], device(b=owner))

    def early_arrival(kind, c, i):
        n, states, _, _ = sides[kind]
        place = states.at[i, at_chunk(c)]
        k = lax.rem(b + low - i, low) - 1
        return remote(place, place, x_send.at[n, c], x_recv.at[n, k, c], device(b=i))

    def late(kind, c, i):
        n, states, _, kept = sides[kind]
        return remote(
            states.at[i, at_chunk(c)],
            kept.at[at_chunk(c)],
            l_send.at[n, lax.rem(i + low - b, low) - 1, c],
            l_recv.at[n, c],
            device(b=i),
        )

    def late_arrival(kind, c):
        n, _, _, kept = sides[kind]
        place = kept.at[at_chunk(c)]
        return remote(place, place, l_send.at[n, 0, c], l_recv.at[n, c], device())

    def needs_early(kind, i, owner):
        last = high - 1 if kind == "F" else 0
        return (i != owner) & ((a != last) | (i != order_of(kind)[-1]))

    def needs_late(kind, i, owner):
        first = 0 if kind == "F" else high - 1
        return (i != owner) & ((a != first) | (i != order_of(kind)[0]))

    def z_copy(kind, c, toward):
        n, _, carried, _ = sides[kind]
        return remote(
            carried.at[at_chunk(c)],
            carried.at[at_chunk(c)],
            z_send.at[n, c],
            z_recv.at[n, c],
            device(a=toward),
        )

    half = HEADS * per_head
    opening = OPENING * per_head

    def chunk_of(kind, slot):
        c = slot if kind == "B" else slot - half
        return c, (c >= 0) & (c < half)

    def issue(slot):
        for kind in ("B", "F"):
            c, asked = chunk_of(kind, slot)
            owner = lax.rem(c + 2 * slots, low)

            @pl.when(asked & needs_early(kind, b, owner))
            def _():
                early(kind, c, owner).start()

    def serve(kind, slot):
        _, states, carried, kept = sides[kind]
        c, asked = chunk_of(kind, slot)
        head = (c + 2 * slots) // per_head - 2 * slots // per_head
        first, last, ahead = (0, high - 1, 1) if kind == "F" else (high - 1, 0, -1)


        @pl.when(asked & (lax.rem(c + 2 * slots, low) == b))
        def _():
            here = at_chunk(c)
            for i in range(low):

                @pl.when(needs_early(kind, i, b))
                def _():
                    early_arrival(kind, c, i).wait_recv()

            @pl.when(a == first)
            def _():
                carried[here, :] = jnp.zeros((step_rows, DK), jnp.float32)

            @pl.when(a != first)
            def _():
                z_copy(kind, c, a).wait_recv()

            current = carried[here, :]
            for i in order_of(kind):
                own = states[i, here, :]
                decay = d_all[i, pl.ds(pl.multiple_of(head * 8, 8), 8), :][0:1, :]

                @pl.when(b == i)
                def _():
                    kept[here, :] = current

                @pl.when(needs_late(kind, i, b))
                def _():
                    states[i, here, :] = current
                    late(kind, c, i).start()

                current = decay * current + own

            @pl.when(a != last)
            def _():
                carried[here, :] = current
                z_copy(kind, c, a + ahead).start()

    def arrived(kind, h):
        _, _, _, kept = sides[kind]

        def one(c, _):
            owner = lax.rem(c, low)
            handed = needs_late(kind, b, owner)

            @pl.when(handed)
            def _():
                late_arrival(kind, c).wait_recv()

            @pl.when((b != owner) & jnp.logical_not(handed))
            def _():
                kept[at_chunk(c), :] = jnp.zeros((step_rows, DK), jnp.float32)

            return 0

        lax.fori_loop(h * per_head, (h + 1) * per_head, one, 0)

    def tick(t):
        slot = t + AHEAD

        @pl.when((slot >= opening) & (slot < half))
        def _():
            issue(slot)

        behind = slot - half

        @pl.when((behind >= 0) & (behind < half))
        def _():
            start, stop = FASTER[0] * behind // FASTER[1], FASTER[0] * (behind + 1) // FASTER[1]
            for extra in range(-(-FASTER[0] // FASTER[1])):

                @pl.when(start + extra < stop)
                def _():
                    issue(half + start + extra)

        serve("B", t - SKEW * (high - 1 - a))
        serve("F", t - SKEW * a)

    def states_of(h):
        cols, wide_cols = cut(h, DK), cut(h, DV)
        for one in inputs(h):
            one.wait()
        ones = triangle(size, True).astype(jnp.bfloat16)
        base = jnp.zeros((1, DK), jnp.float32)
        cums = []
        for n in range(blocks):
            made = exact_sum(ones, lg_ref[n * size : (n + 1) * size, cols]) + base
            base = made[size - 1 :, :]
            cums.append(made)
        cum = jnp.concatenate(cums, axis=0)
        query_up = q_ref[:, cols].astype(jnp.float32) * jnp.exp(cum)
        key_end = k_ref[:, cols].astype(jnp.float32) * jnp.exp(base - cum)
        b_all[b, wide_cols, :] = scale * mm(g_ref[:, wide_cols], query_up, TN)
        f_all[b, wide_cols, :] = mm(v_ref[:, wide_cols], key_end, TN)

    def query_block(n, h):
        cols, wide_cols = cut(h, DK), cut(h, DV)
        at = slice(n * size, (n + 1) * size)
        lower = triangle(size, True)
        cum = exact_sum(lower.astype(jnp.bfloat16), lg_ref[at, cols])
        end = cum[size - 1 :, :]
        middle = cum[size // 2 - 1 : size // 2, :]
        key = k_ref[at, cols].astype(jnp.float32)
        pair = jnp.where(lower, mm(g_ref[at, wide_cols], v_ref[at, wide_cols], NT), 0.0)
        near = jnp.exp(cum - middle) * mm(pair, key * jnp.exp(middle - cum), NN)
        if n > 0:
            near += jnp.exp(cum) * mm(g_ref[at, wide_cols], state_ref[...], NN)
        near_ref[at, cols] = scale * near
        if n < blocks - 1:
            added = mm(v_ref[at, wide_cols], key * jnp.exp(end - cum), TN)
            state_ref[...] = state_ref[...] * jnp.exp(end) + added if n > 0 else added

    def key_block(n, h):
        cols, wide_cols = cut(h, DK), cut(h, DV)
        at = slice(n * size, (n + 1) * size)
        lower = triangle(size, True)
        back = bin_[wide_cols, :] if n == blocks - 1 else back_ref[...]
        cum = exact_sum(lower.astype(jnp.bfloat16), lg_ref[at, cols])
        end = cum[size - 1 :, :]
        middle = cum[size // 2 - 1 : size // 2, :]
        fall = jnp.exp(middle - cum)
        to_end = jnp.exp(end - cum)
        query = q_ref[at, cols].astype(jnp.float32)
        key = k_ref[at, cols].astype(jnp.float32)
        query_rise = (query * jnp.exp(cum - middle)).astype(jnp.bfloat16)
        pair = jnp.where(lower, mm(g_ref[at, wide_cols], v_ref[at, wide_cols], NT), 0.0)
        scores = jnp.where(lower, scale * mm(query_rise, key * fall, NT), 0.0)
        dk = scale * fall * mm(pair, query_rise, TN) + to_end * mm(
            v_ref[at, wide_cols], back, NN
        )
        dv = mm(scores, g_ref[at, wide_cols], TN) + mm(key * to_end, back, NT)
        dk_ref[at, cols] = dk.astype(jnp.bfloat16)
        dv_ref[at, wide_cols] = dv.astype(jnp.bfloat16)
        gate_ref[at, cols] = key * dk
        if n > 0:
            back_ref[...] = back * jnp.exp(end) + scale * mm(
                g_ref[at, wide_cols], query * jnp.exp(cum), TN
            )

    def finish(h):
        cols, wide_cols = cut(h, DK), cut(h, DV)
        arrived("F", h)
        sum_down = triangle(size, True).astype(jnp.bfloat16)
        sum_up = triangle(size, False).astype(jnp.bfloat16)
        state = fin[wide_cols, :]
        far = scale * mm(g_ref[:, wide_cols], state, NN)
        base = jnp.zeros((1, DK), jnp.float32)
        kept = []
        for n in range(blocks):
            at = slice(n * size, (n + 1) * size)
            cum = exact_sum(sum_down, lg_ref[at, cols]) + base
            base = cum[size - 1 :, :]
            dq = near_ref[at, cols] + jnp.exp(cum) * far[at, :]
            dq_ref[at, cols] = dq.astype(jnp.bfloat16)
            kept.append(q_ref[at, cols].astype(jnp.float32) * dq - gate_ref[at, cols])
        last = state * jnp.exp(base) + f_all[b, wide_cols, :]
        tail = jnp.sum(last * bin_[wide_cols, :], axis=0, keepdims=True)
        for n in reversed(range(blocks)):
            sums = exact_sum(sum_up, kept[n]) + tail
            gate_ref[n * size : (n + 1) * size, cols] = sums
            tail = sums[0:1, :]
        result(0, h).start()
        result(3, h).start()

    def inputs(h):
        made = []
        for i, width in enumerate((DK, DK, DV, DV)):
            place = (slice(None), cut(h, width))
            made.append(
                pltpu.make_async_copy(
                    given[i].at[place], (q_ref, k_ref, v_ref, g_ref)[i].at[place], in_sem.at[i, h]
                )
            )
        return made

    def result(i, h):
        source = (dq_ref, dk_ref, dv_ref, gate_ref, w_out)[i]
        place = (slice(None), cut(h, DV if i == 2 else DK))
        return pltpu.make_async_copy(source.at[place], outs[i].at[place], out_sem.at[i, h])

    def slot_of(owner):
        place = {
            "b": owner % low,
            "a": owner // low % high,
            "core": owner // (low * high) % 2,
            "y": owner // (low * high * 2),
        }
        slot = 0
        for axis, bit in stages:
            slot = slot * 2 + (place[axis] >> bit) % 2
        return slot

    tall = min(256, x_ref.shape[1])
    tiles = x_ref.shape[1] // tall

    def weight_tile(i, h):
        total = mm(x_ref[:, i * tall : (i + 1) * tall], dk_ref[:, cut(h, DK)], TN)
        for j in range(tall // rows):
            place = slot_of(i * (tall // rows) + j)
            for e in range(2):
                part[h * 2 + e, place] = total[
                    j * rows : (j + 1) * rows, e * LANES : (e + 1) * LANES
                ]

    count = 1 << len(stages)

    def sum_place(s):
        start = 0
        for e, (axis, bit) in enumerate(stages[:s]):
            start = start + flipped(axis, bit)[1] * (count >> (e + 1))
        axis, bit = stages[s]
        peer, mine = flipped(axis, bit)
        n = count >> (s + 1)
        return start + mine * n, start + (1 - mine) * n, n, count - 2 * n, device(**{axis: peer})

    def sum_copy(h, s):
        _, other, n, offset, target = sum_place(s)
        return remote(
            part.at[h, pl.ds(other, n)],
            got.at[h, pl.ds(offset, n)],
            w_send.at[h, s],
            w_recv.at[h, s],
            target,
        )

    def sum_land(e, s, h):
        own, _, n, offset, _ = sum_place(s)
        h = h * 2 + e
        sum_copy(h, s).wait_recv()
        if s == len(stages) - 1:
            w_out[:, cut(h, LANES)] = part[h, own] + got[h, offset]
            return

        def add(j, _):
            part[h, own + j] = part[h, own + j] + got[h, offset + j]
            return 0

        lax.fori_loop(0, n, add, 0)
        sum_copy(h, s + 1).start()

    def key_done(h):
        result(1, h).start()
        result(2, h).start()

    def sum_begin(h):
        for e in range(2):
            sum_copy(h * 2 + e, 0).start()

    def ticks(eighths):
        return eighths * per_head // 8

    events = []
    for n in range(blocks):
        events.append((ticks(8 + 2 * n), functools.partial(query_block, n)))
    key_at = per_head + SKEW * (high - 1) + ticks(LATE)
    todo = [functools.partial(arrived, "B")]
    todo += [functools.partial(key_block, n) for n in reversed(range(blocks))] + [key_done]
    todo += [functools.partial(weight_tile, i) for i in range(tiles)] + [sum_begin]
    for j, one in enumerate(todo):
        events.append((key_at + ticks(j // 3), one))
    sum_at = events[-1][0]
    for s in range(len(stages)):
        for e in range(2):
            spot = AFTER[min(s, len(AFTER) - 2) if s < len(stages) - 1 else -1][e]
            events.append((sum_at + ticks(spot), functools.partial(sum_land, e, s)))
    events.append((half + key_at, finish))
    events.append((events[-2][0] + 1, lambda h: result(4, h).start()))
    events.sort(key=lambda one: (one[0] % per_head, one[0]))
    periods = HEADS + max(one[0] for one in events) // per_head

    def run_ticks(start, stop):
        if isinstance(stop, int) and stop == 1 + start:
            tick(start)
        else:
            lax.fori_loop(start, stop, lambda t, _: (tick(t), 0)[1], 0)

    def period(p, _):
        done = 0
        for offset, act in events:
            upto = offset % per_head
            if upto > done:
                run_ticks(p * per_head + done, p * per_head + upto)
                done = upto
            h = p - offset // per_head

            @pl.when((h >= 0) & (h < HEADS))
            def _():
                act(h)

        run_ticks(p * per_head + done, (p + 1) * per_head)
        return 0

    all_gates = pltpu.make_async_copy(given[4], lg_ref, in_sem.at[4, 0])
    all_rows = pltpu.make_async_copy(given[5], x_ref, in_sem.at[5, 0])
    all_gates.start()
    for h in range(HEADS):
        for one in inputs(h):
            one.start()
    all_rows.start()
    all_gates.wait()
    for h in range(HEADS):
        total = jnp.sum(lg_ref[:, h * DK : (h + 1) * DK], axis=0, keepdims=True)
        d_all[b, h * 8 : (h + 1) * 8, :] = jnp.broadcast_to(jnp.exp(total), (8, DK))
    states_of(0)
    greeting_done()
    for one in d_copies():
        one.start()
    for h in range(HEADS):
        if h > 0:
            states_of(h)
        for slot in range(h * per_head, min(opening, (h + 1) * per_head)):
            issue(slot)
    for k, p in enumerate(row_from):
        remote(d_all.at[p], d_all.at[p], d_send.at[k], d_recv.at[k], device(b=p)).wait_recv()
    all_rows.wait()
    lax.fori_loop(0, periods, period, 0)

    for one in d_copies():
        one.wait_send()

    def drain(c, _):
        owner = lax.rem(c, low)
        for kind, last, ahead in (("F", high - 1, 1), ("B", 0, -1)):

            @pl.when(needs_early(kind, b, owner))
            def _():
                early(kind, c, owner).wait_send()

            for i in range(low):

                @pl.when((owner == b) & needs_late(kind, i, owner))
                def _():
                    late(kind, c, i).wait_send()

            @pl.when((owner == b) & (a != last))
            def _():
                z_copy(kind, c, a + ahead).wait_send()

        return 0

    lax.fori_loop(0, HEADS * per_head, drain, 0)

    def sent(h, _):
        for s in range(len(stages)):
            for e in range(2):
                sum_copy(h * 2 + e, s).wait_send()
        return 0

    lax.fori_loop(0, HEADS, sent, 0)
    for h in range(HEADS):
        for i in range(5):
            result(i, h).wait()


def settle_kernel(pieces, *refs):
    n = (len(refs) - 2) // 3
    given, outs, held = refs[:n], refs[n : 2 * n], refs[2 * n : 3 * n]
    in_sem, out_sem = refs[3 * n :]

    def moves(i, j):
        size = given[i].shape[0] // pieces
        at = pl.ds(j * size, size)
        return (
            pltpu.make_async_copy(given[i].at[at], held[i].at[at], in_sem.at[i, j]),
            pltpu.make_async_copy(held[i].at[at], outs[i].at[at], out_sem.at[i, j]),
        )

    every = [(i, j) for i in range(n) for j in range(pieces)]
    for i, j in every:
        moves(i, j)[0].start()
    for i, j in every:
        moves(i, j)[0].wait()
        moves(i, j)[1].start()
    for i, j in every:
        moves(i, j)[1].wait()


def shards(counts, queries, key_vectors, value_vectors, grad_output, log_gate, layer_input):
    length = queries.shape[1]
    ranks, count = counts
    f32, bf16 = jnp.float32, jnp.bfloat16
    low = max(d for d in range(1, count + 1) if count % d == 0 and d * d <= count)
    sizes = (ranks // 2, count // low, low)
    model = layer_input.shape[2]
    own_rows = model // (ranks * count)
    chunks = HEADS * DV // (ROWS * max(1, low // 2))
    steps = len(sum_stages(sizes))
    rows = (queries[0], key_vectors[0], value_vectors[0], grad_output[0], log_gate[0])
    outside = pl.BlockSpec(memory_space=pl.ANY)
    state = pltpu.VMEM((HEADS * DV, DK), f32)
    every = pltpu.VMEM((low, HEADS * DV, DK), f32)
    summed = pltpu.VMEM((HEADS * 2, ranks * count, own_rows, LANES), f32)
    dma = pltpu.SemaphoreType.DMA
    peers = max(1, low - 1)
    spread = (length, HEADS * DK)
    values = (length, HEADS * DV)
    shapes = [(spread, bf16), (spread, bf16), (values, bf16), (spread, f32)]
    shapes += [((own_rows, HEADS * DK), f32)]
    grad_q, grad_k, grad_v, grad_gate, grad_key_weight = pl.pallas_call(
        functools.partial(flow_kernel, sizes),
        in_specs=[outside] * 6,
        out_specs=[outside] * 5,
        out_shape=[jax.ShapeDtypeStruct(shape, kind) for shape, kind in shapes],
        scratch_shapes=[pltpu.VMEM(spread, bf16)] * 2
        + [pltpu.VMEM(values, bf16)] * 2
        + [pltpu.VMEM(spread, f32), pltpu.VMEM((length, model), bf16)]
        + [pltpu.VMEM(shape, kind) for shape, kind in shapes]
        + [pltpu.VMEM(spread, f32), state, state]
        + [pltpu.VMEM((low, HEADS * 8, DK), f32), every, every, state, state]
        + [summed, summed, pltpu.VMEM((DV, DK), f32), pltpu.VMEM((DV, DK), f32)]
        + [dma((peers,)), dma((peers,)), dma((2, chunks)), dma((2, peers, chunks))]
        + [dma((2, peers, chunks)), dma((2, chunks)), dma((2, chunks)), dma((2, chunks))]
        + [dma((HEADS * 2, steps)), dma((HEADS * 2, steps)), dma((6, HEADS)), dma((5, HEADS))],
        compiler_params=pltpu.CompilerParams(
            collective_id=0, has_side_effects=True, vmem_limit_bytes=67000000
        ),
        name="flow",
    )(*rows, layer_input[0])
    results = (grad_v, grad_gate, grad_q, grad_k, grad_key_weight)
    pieces = 4
    grad_v, grad_gate, grad_q, grad_k, grad_key_weight = pl.pallas_call(
        functools.partial(settle_kernel, pieces),
        in_specs=[outside] * 5,
        out_specs=[outside] * 5,
        out_shape=[jax.ShapeDtypeStruct(one.shape, one.dtype) for one in results],
        scratch_shapes=[pltpu.VMEM(one.shape, one.dtype) for one in results]
        + [dma((5, pieces)), dma((5, pieces))],
        compiler_params=pltpu.CompilerParams(vmem_limit_bytes=67000000),
        name="settle",
    )(*results)
    return (grad_q[None], grad_k[None], grad_v[None], grad_gate[None], grad_key_weight)


def solution(mesh):
    rows = P("dp", "seq", None)
    return jax.shard_map(
        functools.partial(shards, (mesh.shape["dp"], mesh.shape["seq"])),
        mesh=mesh,
        in_specs=(rows,) * 6,
        out_specs=(rows, rows, rows, rows, P(("dp", "seq"), None)),
        check_vma=False,
    )
```
